16 devices in a mesh: layer: 4 (over z, y), tensor: 4 (over x, core).
Axes of the slice: x: 2, y: 2, z: 2, core: 2. Of those that a mesh axis runs over, the one named last changes fastest.
Arguments:
- gradient: bfloat16 [2048, 6144], P('layer', 'tensor'), parts along dimension 0
- left_stat: float32 [2048, 512], P(('layer', 'tensor')), parts along dimension 0
- right_stat: float32 [24576, 6144], P(('layer', 'tensor')), parts along dimension 0
- left_root: bfloat16 [2048, 512], P(('layer', 'tensor')), parts along dimension 0
- right_root: bfloat16 [24576, 6144], P(('layer', 'tensor')), parts along dimension 0
Outputs:
- output 1: float32 [2048, 512], P(('layer', 'tensor')), parts along dimension 0
- output 2: float32 [24576, 6144], P(('layer', 'tensor')), parts along dimension 0
- output 3: float32 [2048, 6144], P('layer', 'tensor'), parts along dimension 0
There are 4 independent parts. The reference program is written for one: setup_inputs(seed, part) draws one part's arguments, and reference() takes and returns one part's arrays. A program takes and returns all parts, laid end to end along the dimension named above; each array names one.
All inputs are finite; a program needn't handle non-finite values.
Results may differ from the reference program's by a relative error of at most 0.001.
Values are sent between devices in bfloat16 or wider.
A program may use at most 1 GiB of HBM per device.

```python
import jax
import jax.numpy as jnp

ROW_COUNT = 512
COL_COUNT = 6144
EMA_DECAY = 0.9


def setup_inputs(seed: int = 0, part: int = 0) -> dict:
    base_key = jax.random.fold_in(jax.random.key(seed), part)
    keys = jax.random.split(base_key, 5)
    grad_scale = (ROW_COUNT * COL_COUNT) ** -0.25
    root_scale = (ROW_COUNT * COL_COUNT) ** 0.125
    gradient = grad_scale * jax.random.normal(keys[0], (ROW_COUNT, COL_COUNT), jnp.float32)
    left_hist = jax.random.normal(keys[1], (ROW_COUNT, COL_COUNT // 8), jnp.float32)
    left_stat = (0.8 * grad_scale ** 2) * jnp.dot(left_hist, left_hist.T)
    right_hist = jax.random.normal(keys[2], (COL_COUNT, ROW_COUNT // 8), jnp.float32)
    right_stat = (0.8 * grad_scale ** 2) * jnp.dot(right_hist, right_hist.T)
    left_basis = jax.random.normal(keys[3], (ROW_COUNT, ROW_COUNT // 8), jnp.float32)
    left_root = root_scale * (0.5 * jnp.eye(ROW_COUNT, dtype=jnp.float32) + jnp.dot(left_basis, left_basis.T) / ROW_COUNT)
    right_basis = jax.random.normal(keys[4], (COL_COUNT, COL_COUNT // 8), jnp.float32)
    right_prod = jnp.dot(right_basis, right_basis.T) / COL_COUNT
    right_root = root_scale * (0.5 * jnp.eye(COL_COUNT, dtype=jnp.float32) + 0.5 * (right_prod + right_prod.T))
    return {"gradient": gradient.astype(jnp.bfloat16), "left_stat": left_stat, "right_stat": right_stat, "left_root": left_root.astype(jnp.bfloat16), "right_root": right_root.astype(jnp.bfloat16)}


def reference(gradient, left_stat, right_stat, left_root, right_root):
    left_new = EMA_DECAY * left_stat + (1.0 - EMA_DECAY) * jnp.dot(gradient, gradient.T, preferred_element_type=jnp.float32)
    right_new = EMA_DECAY * right_stat + (1.0 - EMA_DECAY) * jnp.dot(gradient.T, gradient, preferred_element_type=jnp.float32)
    precond = jnp.dot(gradient, right_root, preferred_element_type=jnp.float32).astype(jnp.bfloat16)
    direction = jnp.dot(left_root, precond, preferred_element_type=jnp.float32)
    return (left_new, right_new, direction)
```

```python
import functools

import jax
import jax.numpy as jnp
from jax import lax
from jax.experimental import pallas as pl
from jax.experimental.pallas import tpu as pltpu
from jax.sharding import PartitionSpec as P

EMA_DECAY = 0.9
NT = (((1,), (1,)), ((), ()))
CHUNKS = (768, 512, 256)
TILE = 256
IN_SLOTS, OUT_SLOTS = 4, 3


def dot_nt(a, b):
    return lax.dot_general(a, b, NT, preferred_element_type=jnp.float32)


def stats_kernel(sources, first, last, *refs):
    it = iter(refs)
    right, root = next(it), next(it)
    g_srcs = [next(it) for _ in sources]
    if not first:
        gt_ref, xt_in, lacc_in, _ = next(it), next(it), next(it), next(it)
    if last:
        lr_ref, left_ref = next(it), next(it)
    rnew = next(it)
    if first:
        gt_ref = next(it)
    if last:
        lnew_ref, d_ref = next(it), next(it)
    else:
        xt_ref, lacc_ref = next(it), next(it)
    g_buf, r_buf, root_buf, o_buf, g_sem, r_sem, root_sem, o_sem = [next(it) for _ in range(8)]
    if last:
        xt_ref, lacc_ref = next(it), next(it)

    me = lax.axis_index("tensor")
    width = right.shape[0]
    rows = lacc_ref.shape[0]
    counts = [w // TILE for _, _, w in sources]
    n = sum(counts)

    def column(i):
        col, start = 0, 0
        for (bit, c0, w), cnt in zip(sources, counts):
            inside = (i >= start) & (i < start + cnt)
            col = col + jnp.where(inside, (me ^ bit) * width + c0 + (i - start) * TILE, 0)
            start += cnt
        return pl.multiple_of(col, TILE)

    def loads(i, slot):
        cols = pl.ds(column(i), TILE)
        return (
            pltpu.make_async_copy(right.at[:, cols], r_buf.at[slot], r_sem.at[slot]),
            pltpu.make_async_copy(root.at[:, cols], root_buf.at[slot], root_sem.at[slot]),
        )

    def store(i, slot):
        return pltpu.make_async_copy(o_buf.at[slot], rnew.at[:, pl.ds(column(i), TILE)], o_sem.at[slot])

    g_copies, at = [], 0
    for s, (_, _, w) in enumerate(sources):
        g_copies.append(pltpu.make_async_copy(g_srcs[s], g_buf.at[:, pl.ds(at, w)], g_sem.at[s]))
        at += w
    for c in g_copies:
        c.start()
    for i in range(min(IN_SLOTS, n)):
        for c in loads(i, i):
            c.start()
    for c in g_copies:
        c.wait()
    if first:
        gt_ref[...] = g_buf[:, pl.ds(0, width)].T
        xt_ref[...] = jnp.zeros_like(xt_ref)
        lacc_ref[...] = jnp.zeros_like(lacc_ref)
    else:
        xt_ref[...] = xt_in[...]
        lacc_ref[...] = lacc_in[...]

    def step(i, _):
        slot, oslot = lax.rem(i, IN_SLOTS), lax.rem(i, OUT_SLOTS)
        for c in loads(i, slot):
            c.wait()

        @pl.when(i >= OUT_SLOTS)
        def _():
            store(i - OUT_SLOTS, oslot).wait()

        cols = pl.ds(pl.multiple_of(i * TILE, TILE), TILE)
        g = g_buf[:, cols]
        prod = jnp.dot(gt_ref[...], g, preferred_element_type=jnp.float32)
        o_buf[oslot] = EMA_DECAY * r_buf[slot] + (1.0 - EMA_DECAY) * prod
        store(i, oslot).start()
        xt_ref[...] += dot_nt(root_buf[slot], g)
        mine = g_buf[pl.ds(pl.multiple_of(me * rows, rows), rows), cols]
        lacc_ref[...] += dot_nt(mine, g)

        @pl.when(i + IN_SLOTS < n)
        def _():
            for c in loads(i + IN_SLOTS, slot):
                c.start()

        return 0

    lax.fori_loop(0, n, step, 0)
    if last:
        lnew_ref[...] = EMA_DECAY * left_ref[...] + (1.0 - EMA_DECAY) * lacc_ref[...]
        d_ref[...] = dot_nt(lr_ref[...], xt_ref[...].astype(jnp.bfloat16))
    for i in range(max(0, n - OUT_SLOTS), n):
        store(i, i % OUT_SLOTS).wait()


def solution(mesh):
    row_spec = P(("layer", "tensor"), None)
    col_spec = P("layer", "tensor")
    n_tensor = mesh.shape["tensor"]

    def permute(x, bit):
        return lax.ppermute(x, "tensor", [(t, t ^ bit) for t in range(n_tensor)])

    def local_step(grad, left, right, left_root, right_root):
        m, w = grad.shape
        n = right.shape[1]
        lrows = left.shape[0]
        f32 = jnp.float32

        def call(sources, carry, final=None):
            first, last = carry is None, final is not None
            whole = pl.BlockSpec(memory_space=pltpu.VMEM)
            hbm = pl.BlockSpec(memory_space=pl.ANY)
            ins = [right, right_root] + [a for a, _, _ in sources]
            in_specs = [hbm] * len(ins)
            aliases = {}
            if not first:
                rnew, gt, xt, lacc = carry
                ins += [gt, xt, lacc, rnew]
                in_specs += [whole, whole, whole, hbm]
                aliases[len(ins) - 1] = 0
            if last:
                ins += [final, left]
                in_specs += [whole, whole]
            xt_shape, l_shape = jax.ShapeDtypeStruct((w, m), f32), jax.ShapeDtypeStruct((lrows, m), f32)
            outs, out_specs = [jax.ShapeDtypeStruct((w, n), f32)], [hbm]
            if first:
                outs.append(jax.ShapeDtypeStruct((w, m), jnp.bfloat16))
                out_specs.append(whole)
            cols = sum(a.shape[1] for a, _, _ in sources)
            scratch = [
                pltpu.VMEM((m, cols), jnp.bfloat16),
                pltpu.VMEM((IN_SLOTS, w, TILE), f32),
                pltpu.VMEM((IN_SLOTS, w, TILE), jnp.bfloat16),
                pltpu.VMEM((OUT_SLOTS, w, TILE), f32),
                pltpu.SemaphoreType.DMA((len(sources),)),
                pltpu.SemaphoreType.DMA((IN_SLOTS,)),
                pltpu.SemaphoreType.DMA((IN_SLOTS,)),
                pltpu.SemaphoreType.DMA((OUT_SLOTS,)),
            ]
            if last:
                outs += [l_shape, jax.ShapeDtypeStruct((m, w), f32)]
                scratch += [pltpu.VMEM((w, m), f32), pltpu.VMEM((lrows, m), f32)]
            else:
                outs += [xt_shape, l_shape]
            out_specs += [whole, whole]
            info = tuple((bit, c0, a.shape[1]) for a, bit, c0 in sources)
            res = pl.pallas_call(
                functools.partial(stats_kernel, info, first, last),
                out_shape=outs,
                in_specs=in_specs,
                out_specs=out_specs,
                scratch_shapes=scratch,
                input_output_aliases=aliases,
                compiler_params=pltpu.CompilerParams(vmem_limit_bytes=40 << 20),
                cost_estimate=pl.CostEstimate(flops=4 * w * m * cols, bytes_accessed=10 * w * cols, transcendentals=0),
            )(*ins)
            if last:
                return res
            if first:
                return tuple(res)
            return res[0], carry[1], res[1], res[2]

        near = permute(grad, 1)
        far, c0 = [], 0
        for cw in CHUNKS:
            far.append((permute(grad[:, c0:c0 + cw], 2), c0))
            c0 += cw
        relay = [permute(x, 1) for x, _ in far]
        lr_near = permute(left_root, 1)
        lr_far = permute(left_root, 2)
        lr_relay = permute(lr_far, 1)

        carry = call([(grad, 0, 0), (near, 1, 0)], None)
        me = lax.axis_index("tensor")
        final = jnp.zeros((n_tensor * lrows, m), jnp.bfloat16)
        for part, bit in ((left_root, 0), (lr_near, 1), (lr_far, 2), (lr_relay, 3)):
            final = lax.dynamic_update_slice(final, part, ((me ^ bit) * lrows, 0))
        for k, ((x, c0), y) in enumerate(zip(far, relay)):
            srcs = [(x, 2, c0), (y, 3, c0)]
            if k + 1 < len(far):
                carry = call(srcs, carry)
            else:
                rnew, lnew, d = call(srcs, carry, final)
        return lnew, rnew, d

    return jax.shard_map(local_step, mesh=mesh, in_specs=(col_spec, row_spec, row_spec, row_spec, row_spec), out_specs=(row_spec, row_spec, col_spec), check_vma=False)
```
